32 devices in a mesh: occ: 8 (over z, core), aux: 4 (over y, x).
Axes of the slice: x: 2, y: 2, z: 4, core: 2. Of those that a mesh axis runs over, the one named last changes fastest.
Arguments:
- integrals: bfloat16 [2048, 256, 512], P('aux', 'occ'), may hold values from -1.1953125 to 1.1953125
- metric: bfloat16 [2048, 2048], replicated, may hold values from -0.125 to 0.125
- e_occ: float32 [256], replicated, may hold values from -2 to -0.3
- e_vir: float32 [512], replicated, may hold values from 0.2 to 3
- partner: int32 [256, 2], P(('occ', 'aux')), may hold values from 0 to 7
- screen: int32 [256, 2], P(('occ', 'aux')), may hold values from 0 to 1
Outputs:
- gradient: bfloat16 [2048, 256, 512], P(None, ('occ', 'aux'))
- density: float32 [512, 512], P('occ')
The draws below stay inside these ranges and needn't reach their ends.
All inputs are finite; a program needn't handle non-finite values.
Results may differ from the reference program's by a relative error of at most 0.0055.
Values may be sent and summed in bfloat16 or wider, within the bound.
A program may use at most 192 MiB of HBM per device.

```python
import jax
import jax.numpy as jnp
from jax import lax

NOCC = 256
NVIR = 512
NAUX = 2048
ROUNDS = 2
OWN = 8
N_OCC = 8
N_AUX = 4


def draw_screen(key, part):
    first, second = jax.random.split(jax.random.fold_in(key, 17))
    level = jax.random.randint(first, (NOCC // OWN, 1, 1), 1, 5)
    roll = jax.random.randint(second, (NOCC // OWN, OWN, ROUNDS), 0, 4)
    return (roll < level).astype(jnp.int32).reshape(NOCC, ROUNDS)


def touch_ends(entries, rng, low, top_value):
    extent = entries.shape
    place = [jax.random.randint(jax.random.fold_in(rng, axis), (), 0, extent[axis]) for axis in range(len(extent))]
    entries = entries.at[tuple(place)].set(low)
    longest = extent.index(max(extent))
    place[longest] = (place[longest] + 1) % extent[longest]
    return entries.at[tuple(place)].set(top_value)


def level_of(own_key, extent, cuts, smallest, largest):
    def one(dim, parts):
        heights = jax.random.uniform(jax.random.fold_in(jax.random.fold_in(own_key, 6), dim), (parts,), jnp.float32, smallest / len(cuts), largest / len(cuts))
        return jnp.repeat(jnp.exp(heights), extent[dim] // parts).reshape((-1,) + (1,) * (len(extent) - dim - 1))

    gain = one(*cuts[0])
    for cut in cuts[1:]:
        gain = gain * one(*cut)
    return gain


def normal_values(key, extent, spread, most, pieces=(), kind=jnp.bfloat16):
    array = jax.random.normal(key, extent, jnp.float32) * spread
    if len(pieces) > 0:
        array = level_of(key, extent, pieces, -0.22, 0.18) * array
    return jnp.clip(array, min=-most, max=most).astype(kind)


def setup_inputs(seed: int = 0) -> dict:
    keys = jax.random.split(jax.random.key(seed), 7)
    integrals = normal_values(keys[0], (NAUX, NOCC, NVIR), 0.17, 1.1953125, ((0, 4), (1, 8)))
    metric = normal_values(keys[1], (NAUX, NAUX), NAUX ** -0.5, 0.125)
    e_occ = jnp.clip(jax.random.uniform(keys[2], (NOCC,), jnp.float32, -2.0, -0.3), -2.0, -0.3)
    e_vir = jnp.clip(jax.random.uniform(keys[3], (NVIR,), jnp.float32, 0.2, 3.0), 0.2, 3.0)
    partner = touch_ends(jax.random.randint(keys[4], (NOCC, ROUNDS), 0, OWN), jax.random.fold_in(keys[4], 1), 0, OWN - 1).astype(jnp.int32)
    screen = draw_screen(jax.random.fold_in(keys[6], 71), 0)
    return {"integrals": integrals, "metric": metric, "e_occ": e_occ, "e_vir": e_vir, "partner": partner, "screen": screen}


def reference(integrals, metric, e_occ, e_vir, partner, screen):
    groups = N_OCC * N_AUX
    own = NOCC // groups
    flat = integrals.reshape(NAUX, NOCC * NVIR)
    coeff = jnp.dot(metric, flat, preferred_element_type=jnp.float32).astype(jnp.bfloat16).reshape(NAUX, NOCC, NVIR)
    pair_sum = e_vir[:, None] + e_vir[None, :]
    shifts = (1, groups // 2)

    def visit(density, index):
        gamma_row = jnp.zeros((NAUX, NVIR), jnp.float32)
        for rnd in range(ROUNDS):
            source = (index // own - shifts[rnd % 2]) % groups
            other = (source * own + partner[index, rnd]).astype(jnp.int32)
            left = lax.dynamic_index_in_dim(coeff, index, 1, False)
            right = lax.dynamic_index_in_dim(coeff, other, 1, False)
            intersection = lax.dot_general(left, right, (((0,), (0,)), ((), ())), preferred_element_type=jnp.float32)
            gap = pair_sum - e_occ[index] - e_occ[other]
            amp = (screen[index, rnd].astype(jnp.float32) * intersection / gap).astype(jnp.bfloat16)
            gamma_row = gamma_row + lax.dot_general(right, amp, (((1,), (1,)), ((), ())), preferred_element_type=jnp.float32)
            density = density + lax.dot_general(amp, amp, (((1,), (1,)), ((), ())), preferred_element_type=jnp.float32)
        return density, gamma_row.astype(jnp.bfloat16)

    start = jnp.zeros((NVIR, NVIR), jnp.float32)
    density, rows = lax.scan(visit, start, jnp.arange(NOCC, dtype=jnp.int32))
    gradient = jnp.transpose(rows, (1, 0, 2))
    return gradient, density / NOCC
```

```python
import jax
import jax.numpy as jnp
from jax import lax
from jax.sharding import PartitionSpec as P

NOCC = 256
ROUNDS = 2
BOTH = ("occ", "aux")


def passed_along(array, axis, by):
    count = lax.axis_size(axis)
    return lax.ppermute(array, axis, [(i, (i + by) % count) for i in range(count)])


def on_device(integrals, metric, e_occ, e_vir, partner, screen):
    groups = lax.axis_size(BOTH)
    n_aux = lax.axis_size("aux")
    depth, held, nvir = integrals.shape
    own = held // n_aux
    naux = depth * n_aux
    split = integrals.reshape(depth, n_aux, own, nvir)
    device = lax.axis_index(BOTH)
    pair_sum = e_vir[:, None] + e_vir[None, :]
    shifts = [(1, groups // 2)[rnd % 2] for rnd in range(ROUNDS)]

    coeff = []
    arrived = [[None] * own for _ in range(ROUNDS)]
    for slot in range(own):
        piece = jnp.transpose(split[:, :, slot, :], (1, 0, 2))
        if slot > 0:
            piece, _ = lax.optimization_barrier((piece, coeff[slot - 1]))
        moved = lax.all_to_all(piece, "aux", split_axis=0, concat_axis=0, tiled=True)
        mixed = jnp.dot(metric, moved.reshape(naux, nvir), preferred_element_type=jnp.float32)
        block = mixed.astype(jnp.bfloat16)
        coeff.append(block)
        for rnd in reversed(range(ROUNDS)):
            arrived[rnd][slot] = passed_along(block, BOTH, shifts[rnd])

    terms = [None] * own
    density = None
    for rnd in range(ROUNDS):
        source = (device - shifts[rnd]) % groups
        fetched = jnp.stack(arrived[rnd], axis=0)
        amps = []
        for slot in range(own):
            local = partner[slot, rnd]
            kept = screen[slot, rnd].astype(jnp.float32)
            right = lax.dynamic_index_in_dim(fetched, local, 0, False)
            intersection = lax.dot_general(
                coeff[slot], right, (((0,), (0,)), ((), ())), preferred_element_type=jnp.float32
            )
            gap = pair_sum - e_occ[device * own + slot] - e_occ[source * own + local]
            amp = (kept * intersection / gap).astype(jnp.bfloat16)
            amps.append(amp)
            term = lax.dot_general(
                right, amp, (((1,), (1,)), ((), ())), preferred_element_type=jnp.float32
            )
            terms[slot] = term if terms[slot] is None else terms[slot] + term
        for amp in amps:
            part = lax.dot_general(
                amp, amp, (((1,), (1,)), ((), ())), preferred_element_type=jnp.float32
            )
            density = part if density is None else density + part

    rows = density.reshape(groups, nvir // groups, nvir)
    rows = lax.all_to_all(rows, BOTH, split_axis=0, concat_axis=0, tiled=True)
    mine = jnp.sum(rows, axis=0)
    block = lax.all_gather(mine, "aux", axis=0, tiled=True)
    gamma = jnp.stack([term.astype(jnp.bfloat16) for term in terms], axis=1)
    return (gamma, block / NOCC)


def solution(mesh):
    placed = (
        P("aux", "occ", None),
        P(),
        P(),
        P(),
        P(BOTH, None),
        P(BOTH, None),
    )
    return jax.shard_map(
        on_device,
        mesh=mesh,
        in_specs=placed,
        out_specs=(P(None, BOTH, None), P("occ", None)),
        check_vma=False,
    )
```
